512 devices in a mesh: egrp: 32 (over x, z_hi, core), eloc: 16 (over y, z_lo).
Axes of the slice: x: 4, y: 4, z: 16 (z_hi: 4, z_lo: 4; z = z_hi * 4 + z_lo), core: 2. Of those that a mesh axis runs over, the one named last changes fastest.
Arguments:
- green_blocks: bfloat16 [512, 16, 3, 64, 128], P(('egrp', 'eloc')), may hold values from -0.3125 to 0.3125
- sigma_prev: bfloat16 [512, 16, 64, 128], P(('egrp', 'eloc')), may hold values from -6 to 6
- neighbours: int32 [16, 2], replicated, may hold values from 0 to 15
- couplings: bfloat16 [6, 16, 64, 128], P(None, 'eloc'), may hold values from -0.375 to 0.375
- occupancy: float32 [6], replicated, may hold values from 0.1 to 2
- shifts: int32 [6], replicated, may hold values from 1 to 16, as said below
Outputs:
- sigma_next: bfloat16 [512, 16, 64, 128], P(('egrp', 'eloc'))
The draws below stay inside these ranges and needn't reach their ends.
Inputs may be any that keep to these rules, and one draw needn't show every extreme that they name: `shifts`: at least one mode's shift equals 16.
All inputs are finite; a program needn't handle non-finite values.
Results may differ from the reference program's by a relative error of at most 0.0065.
Values may be sent and summed in bfloat16 or wider, within the bound.
A program may use at most 64 MiB of HBM per device.

```python
import math
import jax
import jax.numpy as jnp
from jax import lax

ORB = 64
ATOMS = 16
MODES = 6
GROUP = 16
ENERGIES = 512


def draw_shifts(key, part):
    first_key, second_key = jax.random.split(jax.random.fold_in(key, 11))
    drawn = jax.random.randint(first_key, (MODES,), 1, GROUP + 1)
    picked = jax.random.randint(second_key, (), 0, MODES)
    return jnp.where(jnp.arange(MODES) == picked, GROUP, drawn).astype(jnp.int32)


def plant(values, stream_key, low, largest):
    longest = values.shape.index(max(values.shape))
    spots = []
    for shift in (0, 1):
        where = [jax.random.randint(jax.random.fold_in(stream_key, axis), (), 0, length) for axis, length in enumerate(values.shape)]
        where[longest] = (where[longest] + shift) % values.shape[longest]
        spots.append(tuple(where))
    return values.at[spots[0]].set(low).at[spots[1]].set(largest)


def steps_of(stream_key, extent, shards, least, largest):
    def one(dim, parts):
        draws = jax.random.uniform(jax.random.fold_in(jax.random.fold_in(stream_key, 6), dim), (parts,), jnp.float32, least / len(shards), largest / len(shards))
        return jnp.repeat(jnp.exp(draws), extent[dim] // parts).reshape((-1,) + (1,) * (len(extent) - dim - 1))

    factor_of = one(*shards[0])
    for cut in shards[1:]:
        factor_of = factor_of * one(*cut)
    return factor_of


def scatter_about(own_key, dims, width, bound, pieces=(), kind=jnp.bfloat16):
    entries = jax.random.normal(own_key, dims, jnp.float32) * width
    if len(pieces) > 0:
        entries = steps_of(own_key, dims, pieces, -0.22, 0.18) * entries
    return jnp.clip(entries, min=-bound, max=bound).astype(kind)


def setup_inputs(seed: int = 0) -> dict:
    streams_of = jax.random.split(jax.random.key(seed), 7)
    green_blocks = scatter_about(streams_of[0], (ENERGIES, ATOMS, 3, ORB, 2 * ORB), (6 * ORB) ** -0.5, 0.3125, ((0, 512),))
    sigma_prev = scatter_about(streams_of[1], (ENERGIES, ATOMS, ORB, 2 * ORB), 1.0, 6.0, ((0, 512),))
    neighbours = plant(jax.random.randint(streams_of[2], (ATOMS, 2), 0, ATOMS), jax.random.fold_in(streams_of[2], 1), 0, ATOMS - 1).astype(jnp.int32)
    couplings = scatter_about(streams_of[3], (MODES, ATOMS, ORB, 2 * ORB), (4 * ORB) ** -0.5, 0.375, ((1, 16),))
    occupancy = jnp.clip(jnp.exp(jax.random.uniform(streams_of[4], (MODES,), jnp.float32, math.log(0.1), math.log(2.0))), 0.1, 2.0)
    shifts = draw_shifts(jax.random.fold_in(streams_of[6], 71), 0)
    return {"green_blocks": green_blocks, "sigma_prev": sigma_prev, "neighbours": neighbours, "couplings": couplings, "occupancy": occupancy, "shifts": shifts}


def widened_form(block):
    orbitals = block.shape[-2]
    real_part = block[..., :orbitals]
    imag_part = block[..., orbitals:]
    upper_rows = jnp.concatenate([real_part, imag_part], -1)
    lower_rows = jnp.concatenate([-imag_part, real_part], -1)
    return jnp.concatenate([upper_rows, lower_rows], -2)


def adjoint_form(block):
    orbitals = block.shape[-2]
    real_part = jnp.swapaxes(block[..., :orbitals], -1, -2)
    imag_part = jnp.swapaxes(block[..., orbitals:], -1, -2)
    upper_rows = jnp.concatenate([real_part, -imag_part], -1)
    lower_rows = jnp.concatenate([imag_part, real_part], -1)
    return jnp.concatenate([upper_rows, lower_rows], -2)


def reference(green_blocks, sigma_prev, neighbours, couplings, occupancy, shifts):
    atom_index = jnp.concatenate([jnp.arange(ATOMS, dtype=jnp.int32)[:, None], neighbours.astype(jnp.int32)], 1)

    def lesser_one(operands):
        blocks, sigma_local = operands
        chosen = sigma_local[atom_index]
        half_product = jnp.einsum('akij,akjl->akil', blocks.astype(jnp.float32), widened_form(chosen).astype(jnp.float32)).astype(jnp.bfloat16)
        return jnp.einsum('akij,akjl->ail', half_product.astype(jnp.float32), adjoint_form(blocks).astype(jnp.float32))

    lesser = lax.map(lesser_one, (green_blocks, sigma_prev))

    def sigma_atom(operands):
        column, coupling = operands
        padding = jnp.zeros((GROUP,) + column.shape[1:], jnp.float32)
        padded = jnp.concatenate([padding, column, padding], 0)
        accumulated = jnp.zeros(column.shape, jnp.float32)
        for mode_index in range(MODES):
            shift_now = shifts[mode_index].astype(jnp.int32)
            upper_part = lax.dynamic_slice_in_dim(padded, (GROUP + shift_now).astype(jnp.int32), ENERGIES, 0)
            lower_part = lax.dynamic_slice_in_dim(padded, (GROUP - shift_now).astype(jnp.int32), ENERGIES, 0)
            mixture = (occupancy[mode_index] + 1.0) * upper_part + occupancy[mode_index] * lower_part
            coupling_float = coupling[mode_index].astype(jnp.float32)
            left = jnp.einsum('ij,ejl->eil', coupling_float, widened_form(mixture), precision=lax.Precision.HIGHEST)
            accumulated = accumulated + jnp.einsum('eij,jl->eil', left, adjoint_form(coupling_float), precision=lax.Precision.HIGHEST)
        return accumulated

    by_atom = lax.map(sigma_atom, (jnp.moveaxis(lesser, 1, 0), jnp.moveaxis(couplings, 1, 0)))
    return jnp.moveaxis(by_atom, 0, 1).astype(jnp.bfloat16)
```

```python
import functools

import jax
import jax.numpy as jnp
from jax import lax
from jax.experimental import pallas as pl
from jax.experimental.pallas import tpu as pltpu
from jax.sharding import PartitionSpec as P

MESH = pl.DeviceIdType.MESH
RUN = 4


def signs(shape):
    half = shape[-1] // 2
    lane = lax.broadcasted_iota(jnp.int32, shape, len(shape) - 1)
    return jnp.where(lane < half, -1.0, 1.0).astype(jnp.float32)


def turned(block):
    wide = block.astype(jnp.float32)
    return pltpu.roll(wide, block.shape[-1] // 2, 1) * signs(block.shape)


def kernel(
    groups,
    near_ref,
    occ_ref,
    shift_ref,
    green_hbm,
    sigma_hbm,
    coup_ref,
    out_ref,
    green,
    sigma,
    wide,
    mine,
    ext,
    right,
    left,
    mid,
    res,
    in_sem,
    own_send,
    far_send,
    fwd_send,
    pair_send,
    ret_send,
    ext_recv,
    out_recv,
):
    atoms, orb, lanes = sigma.shape
    size = atoms
    modes = right.shape[0]
    chunk = 4
    run = min(RUN, size // 2)
    grp = lax.axis_index("egrp")
    loc = lax.axis_index("eloc")
    core = grp % 2
    partner = grp + 1 - 2 * core
    other = grp - 1 + 2 * core
    has_other = (other >= 0) & (other < groups)
    here = loc % run

    pieces = atoms // chunk
    loads = [
        pltpu.make_async_copy(
            green_hbm.at[0, pl.ds(p * chunk, chunk)],
            green.at[pl.ds(p * chunk, chunk)],
            in_sem.at[p],
        )
        for p in range(pieces)
    ]
    load_sigma = pltpu.make_async_copy(sigma_hbm.at[0], sigma, in_sem.at[pieces])
    load_sigma.start()
    for load in loads:
        load.start()

    barrier = pltpu.get_barrier_semaphore()

    def greet(i, carry):
        @pl.when(i != loc)
        def _():
            pl.semaphore_signal(
                barrier, inc=1, device_id=(grp, i), device_id_type=MESH
            )

        @pl.when(has_other)
        def _():
            pl.semaphore_signal(
                barrier, inc=1, device_id=(other, i), device_id_type=MESH
            )

        return carry

    lax.fori_loop(0, size, greet, 0)
    pl.semaphore_signal(
        barrier, inc=1, device_id=(partner, loc), device_id_type=MESH
    )

    load_sigma.wait()

    def widen(n, carry):
        block = sigma[n]
        wide[n, :orb] = block
        wide[n, orb:] = turned(block).astype(jnp.bfloat16)
        return carry

    lax.fori_loop(0, atoms, widen, 0, unroll=2)

    def lesser(a, carry):
        total = jnp.zeros((orb, lanes), jnp.float32)
        for k in range(3):
            n = a if k == 0 else near_ref[k - 1, a]
            block = green[a, k]
            half = jnp.dot(
                block, wide[n], preferred_element_type=jnp.float32
            ).astype(jnp.bfloat16)
            form = jnp.concatenate([block, turned(block).astype(jnp.bfloat16)], 0)
            total = total + lax.dot_general(
                half, form, (((1,), (1,)), ((), ())), preferred_element_type=jnp.float32
            )
        mine[a] = total.astype(jnp.bfloat16)
        return carry

    for p in range(pieces):
        loads[p].wait()
        lax.fori_loop(p * chunk, (p + 1) * chunk, lesser, 0, unroll=2)

    @pl.when(has_other)
    def _():
        pl.semaphore_wait(barrier, 2 * size)

    @pl.when(jnp.logical_not(has_other))
    def _():
        pl.semaphore_wait(barrier, size)

    far_base = 2 * size * (1 - core)
    pair_base = 2 * size * core

    def own_copy(a):
        return pltpu.make_async_remote_copy(
            src_ref=mine.at[a],
            dst_ref=ext.at[size + loc],
            send_sem=own_send.at[a],
            recv_sem=ext_recv.at[size + loc],
            device_id=(grp, a),
            device_id_type=MESH,
        )

    def far_copy(a):
        return pltpu.make_async_remote_copy(
            src_ref=mine.at[a],
            dst_ref=ext.at[far_base + loc],
            send_sem=far_send.at[a],
            recv_sem=ext_recv.at[far_base + loc],
            device_id=(other, a),
            device_id_type=MESH,
        )

    def forward_copy(j):
        return pltpu.make_async_remote_copy(
            src_ref=ext.at[size + j],
            dst_ref=ext.at[far_base + j],
            send_sem=fwd_send.at[j],
            recv_sem=ext_recv.at[far_base + j],
            device_id=(other, loc),
            device_id_type=MESH,
        )

    def pair_copy(j):
        return pltpu.make_async_remote_copy(
            src_ref=ext.at[size + j],
            dst_ref=ext.at[pair_base + j],
            send_sem=pair_send.at[j],
            recv_sem=ext_recv.at[pair_base + j],
            device_id=(partner, loc),
            device_id_type=MESH,
        )

    def straight(source, worker):
        rise = source % run - worker % run
        return (rise * (2 * core - 1) >= 0) & (source != worker)

    def arrived(slot):
        pltpu.make_async_remote_copy(
            src_ref=ext.at[slot],
            dst_ref=ext.at[slot],
            send_sem=own_send.at[0],
            recv_sem=ext_recv.at[slot],
            device_id=(partner, loc),
            device_id_type=MESH,
        ).wait_recv()

    def send(t, carry):
        a = (loc + t) % size

        @pl.when(has_other & straight(loc, a))
        def _():
            far_copy(a).start()

        own_copy(a).start()
        return carry

    ext[size + loc] = mine[loc]
    lax.fori_loop(1, size, send, 0)

    for m in range(modes):
        block = coup_ref[m, 0].astype(jnp.float32)
        adjoint = jnp.concatenate([block, turned(coup_ref[m, 0])], 0).T
        right[m, :lanes] = (adjoint * (occ_ref[m] + 1.0)).astype(jnp.bfloat16)
        right[m, lanes:] = (adjoint * occ_ref[m]).astype(jnp.bfloat16)
    low = lax.broadcasted_iota(jnp.int32, (orb, lanes), 1) < orb
    for m in range(0, modes, 2):
        one = coup_ref[m, 0].astype(jnp.float32)
        two = coup_ref[m + 1, 0].astype(jnp.float32)
        span = slice(m * orb, m * orb + lanes)
        left[:orb, span] = jnp.where(low, one, pltpu.roll(two, orb, 1)).astype(
            jnp.bfloat16
        )
        left[orb:, span] = jnp.where(low, pltpu.roll(one, orb, 1), two).astype(
            jnp.bfloat16
        )

    def relay(t, carry):
        j = (loc + size - t) % size

        @pl.when(t > 0)
        def _():
            arrived(size + j)

        @pl.when(has_other & jnp.logical_not(straight(j, loc)))
        def _():
            forward_copy(j).start()

        pair_copy(j).start()
        return carry

    lax.fori_loop(0, size, relay, 0)

    def halo(j, carry):
        arrived(pair_other + j)

        @pl.when(has_other)
        def _():
            arrived(far_other + j)

        return carry

    pair_other = 2 * size * (1 - core)
    far_other = 2 * size * core
    lax.fori_loop(0, size, halo, 0)

    @pl.when(jnp.logical_not(has_other))
    def _():
        ext[pl.ds(far_other, size)] = jnp.zeros((size, orb, lanes), ext.dtype)

    def ret_copy(i):
        return pltpu.make_async_remote_copy(
            src_ref=res.at[i],
            dst_ref=out_ref.at[0, loc],
            send_sem=ret_send.at[i],
            recv_sem=out_recv.at[loc],
            device_id=(grp, i),
            device_id_type=MESH,
        )

    def mix(q, carry):
        first = ((loc // run + q) % pieces) * chunk
        for m in range(modes):
            above = ext[pl.ds(size + first + shift_ref[m], chunk)]
            below = ext[pl.ds(size + first - shift_ref[m], chunk)]
            both = jnp.concatenate(
                [above.reshape(chunk * orb, lanes), below.reshape(chunk * orb, lanes)], 1
            )
            product = jnp.dot(both, right[m], preferred_element_type=jnp.float32)
            mid[:, m * orb : (m + 1) * orb] = product.astype(jnp.bfloat16).reshape(
                chunk, orb, lanes
            )
        for i in range(chunk):
            parts = jnp.dot(left[...], mid[i], preferred_element_type=jnp.float32)
            value = parts[:orb] + pltpu.roll(parts[orb:], orb, 1) * signs((orb, lanes))
            res[first + i] = value.astype(jnp.bfloat16)
        for i in range(chunk):

            @pl.when(first + i != loc)
            def _():
                ret_copy(first + i).start()

        return carry

    lax.fori_loop(0, pieces, mix, 0)
    out_ref[0, loc] = res[loc]

    def settle(i, carry):
        @pl.when(i != loc)
        def _():
            pltpu.make_async_remote_copy(
                src_ref=res.at[i],
                dst_ref=out_ref.at[0, i],
                send_sem=ret_send.at[i],
                recv_sem=out_recv.at[i],
                device_id=(grp, i),
                device_id_type=MESH,
            ).wait()
            own_copy(i).wait_send()

        @pl.when(has_other & straight(loc, i))
        def _():
            far_copy(i).wait_send()

        @pl.when(has_other & jnp.logical_not(straight(i, loc)))
        def _():
            forward_copy(i).wait_send()

        pair_copy(i).wait_send()
        return carry

    lax.fori_loop(0, size, settle, 0)


def solution(mesh):
    groups = mesh.shape["egrp"]

    def step(green_blocks, sigma_prev, neighbours, couplings, occupancy, shifts):
        _, atoms, hops, orb, lanes = green_blocks.shape
        modes = couplings.shape[0]
        size = atoms
        vmem = pl.BlockSpec(memory_space=pltpu.VMEM)
        smem = pl.BlockSpec(memory_space=pltpu.SMEM)
        hbm = pl.BlockSpec(memory_space=pl.ANY)
        half = jnp.bfloat16
        return pl.pallas_call(
            functools.partial(kernel, groups),
            out_shape=jax.ShapeDtypeStruct((1, atoms, orb, lanes), half),
            in_specs=[smem, smem, smem, hbm, hbm, vmem],
            out_specs=vmem,
            scratch_shapes=[
                pltpu.VMEM((atoms, hops, orb, lanes), half),
                pltpu.VMEM((atoms, orb, lanes), half),
                pltpu.VMEM((atoms, lanes, lanes), half),
                pltpu.VMEM((atoms, orb, lanes), half),
                pltpu.VMEM((3 * size, orb, lanes), half),
                pltpu.VMEM((modes, 2 * lanes, lanes), half),
                pltpu.VMEM((lanes, modes * orb), half),
                pltpu.VMEM((4, modes * orb, lanes), half),
                pltpu.VMEM((size, orb, lanes), half),
                pltpu.SemaphoreType.DMA((atoms // 4 + 1,)),
                pltpu.SemaphoreType.DMA((size,)),
                pltpu.SemaphoreType.DMA((size,)),
                pltpu.SemaphoreType.DMA((size,)),
                pltpu.SemaphoreType.DMA((size,)),
                pltpu.SemaphoreType.DMA((size,)),
                pltpu.SemaphoreType.DMA((3 * size,)),
                pltpu.SemaphoreType.DMA((size,)),
            ],
            compiler_params=pltpu.CompilerParams(
                collective_id=0, has_side_effects=True
            ),
        )(neighbours.T, occupancy, shifts, green_blocks, sigma_prev, couplings)

    return jax.shard_map(
        step,
        mesh=mesh,
        in_specs=(
            P(("egrp", "eloc"), None, None, None, None),
            P(("egrp", "eloc"), None, None, None),
            P(),
            P(None, "eloc", None, None),
            P(),
            P(),
        ),
        out_specs=P(("egrp", "eloc"), None, None, None),
        check_vma=False,
    )
```

```python
import functools

import jax
import jax.numpy as jnp
from jax import lax
from jax.experimental import pallas as pl
from jax.experimental.pallas import tpu as pltpu
from jax.sharding import PartitionSpec as P

MESH = pl.DeviceIdType.MESH
RUN = 4


def signs(shape):
    half = shape[-1] // 2
    lane = lax.broadcasted_iota(jnp.int32, shape, len(shape) - 1)
    return jnp.where(lane < half, -1.0, 1.0).astype(jnp.float32)


def turned(block):
    wide = block.astype(jnp.float32)
    return pltpu.roll(wide, block.shape[-1] // 2, 1) * signs(block.shape)


def kernel(
    groups,
    near_hbm,
    occ_hbm,
    shift_hbm,
    green_hbm,
    sigma_hbm,
    coup_hbm,
    out_ref,
    near_ref,
    occ_ref,
    shift_ref,
    green,
    sigma,
    coup_ref,
    wide,
    mine,
    ext,
    right,
    left,
    mid,
    res,
    in_sem,
    own_send,
    far_send,
    fwd_send,
    pair_send,
    ret_send,
    ext_recv,
    out_recv,
):
    atoms, orb, lanes = sigma.shape
    size = atoms
    modes = right.shape[0]
    chunk = 4
    lag = min(4, size // 2)
    run = min(RUN, size // 2)
    grp = lax.axis_index("egrp")
    loc = lax.axis_index("eloc")
    core = grp % 2
    partner = grp + 1 - 2 * core
    other = grp - 1 + 2 * core
    has_other = (other >= 0) & (other < groups)
    here = loc % run

    pieces = atoms // chunk

    def turn(t):
        return (loc + t) % size

    def load_green(t):
        return pltpu.make_async_copy(
            green_hbm.at[0, turn(t)], green.at[turn(t)], in_sem.at[t - 1]
        )

    load_near = pltpu.make_async_copy(near_hbm, near_ref, in_sem.at[atoms])
    load_sigma = pltpu.make_async_copy(sigma_hbm.at[0], sigma, in_sem.at[atoms + 1])
    load_occ = pltpu.make_async_copy(occ_hbm, occ_ref, in_sem.at[atoms + 2])
    load_shift = pltpu.make_async_copy(shift_hbm, shift_ref, in_sem.at[atoms + 3])
    load_coup = pltpu.make_async_copy(coup_hbm, coup_ref, in_sem.at[atoms + 4])
    load_sigma.start()
    load_near.start()

    def fetch(t, carry):
        load_green(t).start()
        return carry

    lax.fori_loop(1, size + 1, fetch, 0)
    load_coup.start()
    load_occ.start()
    load_shift.start()

    barrier = pltpu.get_barrier_semaphore()

    def greet(i, carry):
        @pl.when(i != loc)
        def _():
            pl.semaphore_signal(
                barrier, inc=1, device_id=(grp, i), device_id_type=MESH
            )

        @pl.when(has_other)
        def _():
            pl.semaphore_signal(
                barrier, inc=1, device_id=(other, i), device_id_type=MESH
            )

        return carry

    lax.fori_loop(0, size, greet, 0)
    pl.semaphore_signal(
        barrier, inc=1, device_id=(partner, loc), device_id_type=MESH
    )

    load_near.wait()
    load_sigma.wait()

    def widen(n, carry):
        block = sigma[n]
        wide[n, :orb] = block
        wide[n, orb:] = turned(block).astype(jnp.bfloat16)
        return carry

    lax.fori_loop(0, atoms, widen, 0, unroll=2)

    def lesser(t):
        load_green(t).wait()
        a = turn(t)
        total = jnp.zeros((orb, lanes), jnp.float32)
        for k in range(3):
            n = a if k == 0 else near_ref[k - 1, a]
            block = green[a, k]
            half = jnp.dot(
                block, wide[n], preferred_element_type=jnp.float32
            ).astype(jnp.bfloat16)
            form = jnp.concatenate([block, turned(block).astype(jnp.bfloat16)], 0)
            total = total + lax.dot_general(
                half, form, (((1,), (1,)), ((), ())), preferred_element_type=jnp.float32
            )
        mine[a] = total.astype(jnp.bfloat16)

    def first(t, carry):
        lesser(2 * t + 1)
        lesser(2 * t + 2)
        return carry

    lax.fori_loop(0, lag // 2, first, 0)

    @pl.when(has_other)
    def _():
        pl.semaphore_wait(barrier, 2 * size)

    @pl.when(jnp.logical_not(has_other))
    def _():
        pl.semaphore_wait(barrier, size)

    far_base = 2 * size * (1 - core)
    pair_base = 2 * size * core

    def own_copy(a):
        return pltpu.make_async_remote_copy(
            src_ref=mine.at[a],
            dst_ref=ext.at[size + loc],
            send_sem=own_send.at[a],
            recv_sem=ext_recv.at[size + loc],
            device_id=(grp, a),
            device_id_type=MESH,
        )

    def far_copy(a):
        return pltpu.make_async_remote_copy(
            src_ref=mine.at[a],
            dst_ref=ext.at[far_base + loc],
            send_sem=far_send.at[a],
            recv_sem=ext_recv.at[far_base + loc],
            device_id=(other, a),
            device_id_type=MESH,
        )

    def forward_copy(j):
        return pltpu.make_async_remote_copy(
            src_ref=ext.at[size + j],
            dst_ref=ext.at[far_base + j],
            send_sem=fwd_send.at[j],
            recv_sem=ext_recv.at[far_base + j],
            device_id=(other, loc),
            device_id_type=MESH,
        )

    def pair_copy(j):
        return pltpu.make_async_remote_copy(
            src_ref=ext.at[size + j],
            dst_ref=ext.at[pair_base + j],
            send_sem=pair_send.at[j],
            recv_sem=ext_recv.at[pair_base + j],
            device_id=(partner, loc),
            device_id_type=MESH,
        )

    def straight(source, worker):
        rise = source % run - worker % run
        return rise * (2 * core - 1) > 0

    def arrived(slot):
        pltpu.make_async_remote_copy(
            src_ref=ext.at[slot],
            dst_ref=ext.at[slot],
            send_sem=own_send.at[0],
            recv_sem=ext_recv.at[slot],
            device_id=(partner, loc),
            device_id_type=MESH,
        ).wait_recv()

    def send(t):
        a = turn(t)

        @pl.when(has_other & straight(loc, a))
        def _():
            far_copy(a).start()

        own_copy(a).start()

    def later(t, carry):
        send(2 * t + 1 - lag)
        send(2 * t + 2 - lag)
        lesser(2 * t + 1)
        lesser(2 * t + 2)
        return carry

    def last(t, carry):
        send(t)
        return carry

    lax.fori_loop(lag // 2, size // 2, later, 0)
    lax.fori_loop(size - lag + 1, size, last, 0)
    ext[size + loc] = mine[loc]

    def relay(t, carry):
        j = (loc + size - t) % size

        @pl.when(t > 0)
        def _():
            arrived(size + j)

        @pl.when(has_other & jnp.logical_not(straight(j, loc)))
        def _():
            forward_copy(j).start()

        pair_copy(j).start()
        return carry

    lax.fori_loop(0, size, relay, 0)

    load_coup.wait()
    load_occ.wait()
    load_shift.wait()
    for m in range(modes):
        block = coup_ref[m, 0].astype(jnp.float32)
        adjoint = jnp.concatenate([block, turned(coup_ref[m, 0])], 0).T
        right[m, :lanes] = (adjoint * (occ_ref[m] + 1.0)).astype(jnp.bfloat16)
        right[m, lanes:] = (adjoint * occ_ref[m]).astype(jnp.bfloat16)
    low = lax.broadcasted_iota(jnp.int32, (orb, lanes), 1) < orb
    for m in range(0, modes, 2):
        one = coup_ref[m, 0].astype(jnp.float32)
        two = coup_ref[m + 1, 0].astype(jnp.float32)
        span = slice(m * orb, m * orb + lanes)
        left[:orb, span] = jnp.where(low, one, pltpu.roll(two, orb, 1)).astype(
            jnp.bfloat16
        )
        left[orb:, span] = jnp.where(low, pltpu.roll(one, orb, 1), two).astype(
            jnp.bfloat16
        )

    def halo(j, carry):
        arrived(pair_other + j)

        @pl.when(has_other)
        def _():
            arrived(far_other + j)

        return carry

    pair_other = 2 * size * (1 - core)
    far_other = 2 * size * core
    lax.fori_loop(0, size, halo, 0)

    @pl.when(jnp.logical_not(has_other))
    def _():
        ext[pl.ds(far_other, size)] = jnp.zeros((size, orb, lanes), ext.dtype)

    def ret_copy(i):
        return pltpu.make_async_remote_copy(
            src_ref=res.at[i],
            dst_ref=out_ref.at[0, loc],
            send_sem=ret_send.at[i],
            recv_sem=out_recv.at[loc],
            device_id=(grp, i),
            device_id_type=MESH,
        )

    def mix(q, carry):
        first = ((loc // run + q) % pieces) * chunk
        for m in range(modes):
            above = ext[pl.ds(size + first + shift_ref[m], chunk)]
            below = ext[pl.ds(size + first - shift_ref[m], chunk)]
            both = jnp.concatenate(
                [above.reshape(chunk * orb, lanes), below.reshape(chunk * orb, lanes)], 1
            )
            product = jnp.dot(both, right[m], preferred_element_type=jnp.float32)
            mid[:, m * orb : (m + 1) * orb] = product.astype(jnp.bfloat16).reshape(
                chunk, orb, lanes
            )
        for i in range(chunk):
            parts = jnp.dot(left[...], mid[i], preferred_element_type=jnp.float32)
            value = parts[:orb] + pltpu.roll(parts[orb:], orb, 1) * signs((orb, lanes))
            res[first + i] = value.astype(jnp.bfloat16)
        for i in range(chunk):

            @pl.when(first + i != loc)
            def _():
                ret_copy(first + i).start()

        return carry

    lax.fori_loop(0, pieces, mix, 0)
    out_ref[0, loc] = res[loc]

    def settle(i, carry):
        @pl.when(i != loc)
        def _():
            pltpu.make_async_remote_copy(
                src_ref=res.at[i],
                dst_ref=out_ref.at[0, i],
                send_sem=ret_send.at[i],
                recv_sem=out_recv.at[i],
                device_id=(grp, i),
                device_id_type=MESH,
            ).wait()
            own_copy(i).wait_send()

        @pl.when(has_other & straight(loc, i))
        def _():
            far_copy(i).wait_send()

        @pl.when(has_other & jnp.logical_not(straight(i, loc)))
        def _():
            forward_copy(i).wait_send()

        pair_copy(i).wait_send()
        return carry

    lax.fori_loop(0, size, settle, 0)


def solution(mesh):
    groups = mesh.shape["egrp"]

    def step(green_blocks, sigma_prev, neighbours, couplings, occupancy, shifts):
        _, atoms, hops, orb, lanes = green_blocks.shape
        modes = couplings.shape[0]
        size = atoms
        vmem = pl.BlockSpec(memory_space=pltpu.VMEM)
        hbm = pl.BlockSpec(memory_space=pl.ANY)
        half = jnp.bfloat16
        return pl.pallas_call(
            functools.partial(kernel, groups),
            out_shape=pltpu.VMEM((1, atoms, orb, lanes), half),
            in_specs=[hbm] * 6,
            out_specs=vmem,
            scratch_shapes=[
                pltpu.SMEM(neighbours.shape[::-1], jnp.int32),
                pltpu.SMEM((modes,), jnp.float32),
                pltpu.SMEM((modes,), jnp.int32),
                pltpu.VMEM((atoms, hops, orb, lanes), half),
                pltpu.VMEM((atoms, orb, lanes), half),
                pltpu.VMEM(couplings.shape, half),
                pltpu.VMEM((atoms, lanes, lanes), half),
                pltpu.VMEM((atoms, orb, lanes), half),
                pltpu.VMEM((3 * size, orb, lanes), half),
                pltpu.VMEM((modes, 2 * lanes, lanes), half),
                pltpu.VMEM((lanes, modes * orb), half),
                pltpu.VMEM((4, modes * orb, lanes), half),
                pltpu.VMEM((size, orb, lanes), half),
                pltpu.SemaphoreType.DMA((atoms + 5,)),
                pltpu.SemaphoreType.DMA((size,)),
                pltpu.SemaphoreType.DMA((size,)),
                pltpu.SemaphoreType.DMA((size,)),
                pltpu.SemaphoreType.DMA((size,)),
                pltpu.SemaphoreType.DMA((size,)),
                pltpu.SemaphoreType.DMA((3 * size,)),
                pltpu.SemaphoreType.DMA((size,)),
            ],
            compiler_params=pltpu.CompilerParams(
                collective_id=0, has_side_effects=True
            ),
        )(neighbours.T, occupancy, shifts, green_blocks, sigma_prev, couplings)

    return jax.shard_map(
        step,
        mesh=mesh,
        in_specs=(
            P(("egrp", "eloc"), None, None, None, None),
            P(("egrp", "eloc"), None, None, None),
            P(),
            P(None, "eloc", None, None),
            P(),
            P(),
        ),
        out_specs=P(("egrp", "eloc"), None, None, None),
        check_vma=False,
    )
```

```python
import functools

import jax
import jax.numpy as jnp
from jax import lax
from jax.experimental import pallas as pl
from jax.experimental.pallas import tpu as pltpu
from jax.sharding import PartitionSpec as P

MESH = pl.DeviceIdType.MESH
RUN = 4


def signs(shape):
    half = shape[-1] // 2
    lane = lax.broadcasted_iota(jnp.int32, shape, len(shape) - 1)
    return jnp.where(lane < half, -1.0, 1.0).astype(jnp.float32)


def turned(block):
    wide = block.astype(jnp.float32)
    return pltpu.roll(wide, block.shape[-1] // 2, 1) * signs(block.shape)


def kernel(
    groups,
    near_hbm,
    occ_hbm,
    shift_hbm,
    green_hbm,
    sigma_hbm,
    coup_hbm,
    out_ref,
    near_ref,
    occ_ref,
    shift_ref,
    green,
    sigma,
    coup_ref,
    wide,
    mine,
    own,
    ext,
    right,
    left,
    mid,
    res,
    given,
    part,
    in_sem,
    own_send,
    far_send,
    fwd_send,
    pair_send,
    ret_send,
    ext_recv,
    out_recv,
    give_send,
    part_recv,
    far_sem,
    all_sem,
):
    atoms, orb, lanes = sigma.shape
    size = atoms
    modes = right.shape[0]
    chunk = 4
    lag = min(4, size // 2)
    run = min(RUN, size // 2)
    grp = lax.axis_index("egrp")
    loc = lax.axis_index("eloc")
    core = grp % 2
    partner = grp + 1 - 2 * core
    other = grp - 1 + 2 * core
    has_other = (other >= 0) & (other < groups)
    here = loc % run

    pieces = atoms // chunk

    def turn(t):
        return (loc + t) % size

    def load_green(t):
        return pltpu.make_async_copy(
            green_hbm.at[0, turn(t)], green.at[turn(t)], in_sem.at[t - 1]
        )

    load_near = pltpu.make_async_copy(near_hbm, near_ref, in_sem.at[atoms])
    load_sigma = pltpu.make_async_copy(sigma_hbm.at[0], sigma, in_sem.at[atoms + 1])
    load_occ = pltpu.make_async_copy(occ_hbm, occ_ref, in_sem.at[atoms + 2])
    load_shift = pltpu.make_async_copy(shift_hbm, shift_ref, in_sem.at[atoms + 3])
    load_coup = pltpu.make_async_copy(coup_hbm, coup_ref, in_sem.at[atoms + 4])
    load_sigma.start()
    load_near.start()

    def fetch(t, carry):
        load_green(t).start()
        return carry

    lax.fori_loop(1, size + 1, fetch, 0)
    load_coup.start()
    load_occ.start()
    load_shift.start()

    def straight(source, worker):
        rise = source % run - worker % run
        return rise * (2 * core - 1) > 0

    def exports(worker):
        return worker % run // (run // 2) != core

    exporter = has_other & exports(loc)
    importer = has_other & jnp.logical_not(exports(loc))

    def reaches(i):
        return straight(loc, i) | (i == loc)

    hi = (grp // 2) % 4
    lead = jnp.where(core == 1, jnp.where(hi == 3, 0, 1), jnp.where(hi == 0, 1, 0))
    nearer = (core * here + (1 - core) * (run - 1 - here)) * (size // run)
    barrier = pltpu.get_barrier_semaphore()

    def greet(i, carry):
        @pl.when(i != loc)
        def _():
            pl.semaphore_signal(
                barrier, inc=1, device_id=(grp, i), device_id_type=MESH
            )

        @pl.when(has_other & (lead == 1) & reaches(i))
        def _():
            pl.semaphore_signal(
                barrier, inc=1, device_id=(other, i), device_id_type=MESH
            )

        return carry

    lax.fori_loop(0, size, greet, 0)
    pl.semaphore_signal(
        barrier, inc=1, device_id=(partner, loc), device_id_type=MESH
    )

    own[pl.ds(0, size)] = jnp.zeros((size, orb, lanes), own.dtype)
    own[pl.ds(2 * size, size)] = jnp.zeros((size, orb, lanes), own.dtype)
    load_near.wait()
    load_sigma.wait()

    def widen(n, carry):
        block = sigma[n]
        wide[n, :orb] = block
        wide[n, orb:] = turned(block).astype(jnp.bfloat16)
        return carry

    lax.fori_loop(0, atoms, widen, 0, unroll=2)

    def lesser(t):
        load_green(t).wait()
        a = turn(t)
        total = jnp.zeros((orb, lanes), jnp.float32)
        for k in range(3):
            n = a if k == 0 else near_ref[k - 1, a]
            block = green[a, k]
            half = jnp.dot(
                block, wide[n], preferred_element_type=jnp.float32
            ).astype(jnp.bfloat16)
            form = jnp.concatenate([block, turned(block).astype(jnp.bfloat16)], 0)
            total = total + lax.dot_general(
                half, form, (((1,), (1,)), ((), ())), preferred_element_type=jnp.float32
            )
        mine[a] = total.astype(jnp.bfloat16)

    def first(t, carry):
        lesser(2 * t + 1)
        lesser(2 * t + 2)
        return carry

    lax.fori_loop(0, lag // 2, first, 0)

    @pl.when(has_other & (lead == 0))
    def _():
        pl.semaphore_wait(barrier, size + 1 + nearer)

        def answer(i, carry):
            @pl.when(reaches(i))
            def _():
                pl.semaphore_signal(
                    far_sem, inc=1, device_id=(other, i), device_id_type=MESH
                )

            return carry

        lax.fori_loop(0, size, answer, 0)

    @pl.when(jnp.logical_not(has_other & (lead == 0)))
    def _():
        pl.semaphore_wait(barrier, size)

    far_base = 2 * size * (1 - core)
    pair_base = 2 * size * core

    def own_copy(a):
        return pltpu.make_async_remote_copy(
            src_ref=mine.at[a],
            dst_ref=own.at[size + loc],
            send_sem=own_send.at[a],
            recv_sem=ext_recv.at[size + loc],
            device_id=(grp, a),
            device_id_type=MESH,
        )

    def far_copy(a):
        return pltpu.make_async_remote_copy(
            src_ref=mine.at[a],
            dst_ref=ext.at[far_base + loc],
            send_sem=far_send.at[a],
            recv_sem=ext_recv.at[far_base + loc],
            device_id=(other, a),
            device_id_type=MESH,
        )

    def forward_copy(j):
        return pltpu.make_async_remote_copy(
            src_ref=own.at[size + j],
            dst_ref=ext.at[far_base + j],
            send_sem=fwd_send.at[j],
            recv_sem=ext_recv.at[far_base + j],
            device_id=(other, loc),
            device_id_type=MESH,
        )

    def pair_copy(j):
        return pltpu.make_async_remote_copy(
            src_ref=own.at[size + j],
            dst_ref=ext.at[pair_base + j],
            send_sem=pair_send.at[j],
            recv_sem=ext_recv.at[pair_base + j],
            device_id=(partner, loc),
            device_id_type=MESH,
        )

    def arrived(slot):
        pltpu.make_async_remote_copy(
            src_ref=ext.at[slot],
            dst_ref=ext.at[slot],
            send_sem=own_send.at[0],
            recv_sem=ext_recv.at[slot],
            device_id=(partner, loc),
            device_id_type=MESH,
        ).wait_recv()

    def send(t):
        a = turn(t)

        @pl.when(has_other & (lead == 0) & straight(loc, a) & exports(a))
        def _():
            far_copy(a).start()

        own_copy(a).start()

    def later(t, carry):
        send(2 * t + 1 - lag)
        send(2 * t + 2 - lag)
        lesser(2 * t + 1)
        lesser(2 * t + 2)
        return carry

    def last(t, carry):
        send(t)
        return carry

    lax.fori_loop(lag // 2, size // 2, later, 0)
    lax.fori_loop(size - lag + 1, size, last, 0)
    own[size + loc] = mine[loc]

    def source(t):
        return (loc + size - t) % size

    def forward(t):
        @pl.when(exporter & jnp.logical_not(straight(source(t), loc)))
        def _():
            forward_copy(source(t)).start()

    def early(t, carry):
        @pl.when(t > 0)
        def _():
            arrived(size + source(t))

        @pl.when(lead == 0)
        def _():
            forward(t)

        pair_copy(source(t)).start()
        return carry

    def late(t, carry):
        arrived(size + source(t))
        forward(t)
        pair_copy(source(t)).start()
        return carry

    lax.fori_loop(0, size // 2, early, 0)

    @pl.when(has_other & (lead == 1))
    def _():
        pl.semaphore_wait(far_sem, 1 + nearer)
        pl.semaphore_signal(
            all_sem, inc=1, device_id=(other, loc), device_id_type=MESH
        )

        def direct(t, carry):
            @pl.when(straight(loc, turn(t)) & exports(turn(t)))
            def _():
                far_copy(turn(t)).start()

            return carry

        def delayed(t, carry):
            forward(t)
            return carry

        lax.fori_loop(1, size, direct, 0)
        lax.fori_loop(0, size // 2, delayed, 0)

    lax.fori_loop(size // 2, size, late, 0)

    load_coup.wait()
    load_occ.wait()
    load_shift.wait()
    for m in range(modes):
        block = coup_ref[m, 0].astype(jnp.float32)
        adjoint = jnp.concatenate([block, turned(coup_ref[m, 0])], 0).T
        right[m, :lanes] = (adjoint * (occ_ref[m] + 1.0)).astype(jnp.bfloat16)
        right[m, lanes:] = (adjoint * occ_ref[m]).astype(jnp.bfloat16)
    low = lax.broadcasted_iota(jnp.int32, (orb, lanes), 1) < orb
    for m in range(0, modes, 2):
        one = coup_ref[m, 0].astype(jnp.float32)
        two = coup_ref[m + 1, 0].astype(jnp.float32)
        span = slice(m * orb, m * orb + lanes)
        left[:orb, span] = jnp.where(low, one, pltpu.roll(two, orb, 1)).astype(
            jnp.bfloat16
        )
        left[orb:, span] = jnp.where(low, pltpu.roll(one, orb, 1), two).astype(
            jnp.bfloat16
        )

    ext[pl.ds(size, size)] = own[pl.ds(size, size)]

    @pl.when(has_other & (lead == 0))
    def _():
        pl.semaphore_wait(all_sem, 1)

    def give_copy(i):
        return pltpu.make_async_remote_copy(
            src_ref=given.at[i],
            dst_ref=part.at[loc],
            send_sem=give_send.at[i],
            recv_sem=part_recv.at[loc],
            device_id=(other, i),
            device_id_type=MESH,
        )

    def finish(m_blocks, target, first):
        for i in range(chunk):
            parts = jnp.dot(left[...], m_blocks[i], preferred_element_type=jnp.float32)
            value = parts[:orb] + pltpu.roll(parts[orb:], orb, 1) * signs((orb, lanes))
            target[first + i] = value.astype(jnp.bfloat16)

    @pl.when(importer)
    def _():
        def give(q, carry):
            first = ((loc // run + q) % pieces) * chunk
            for m in range(modes):
                start = first + shift_ref[m] + core * (2 * size - 2 * shift_ref[m])
                block = own[pl.ds(start, chunk)].reshape(chunk * orb, lanes)
                product = jnp.dot(
                    block,
                    right[m, pl.ds(core * lanes, lanes)],
                    preferred_element_type=jnp.float32,
                )
                mid[:, m * orb : (m + 1) * orb] = product.astype(
                    jnp.bfloat16
                ).reshape(chunk, orb, lanes)
            finish(mid, given, first)
            for i in range(chunk):
                give_copy(first + i).start()
            return carry

        lax.fori_loop(0, pieces, give, 0)

    def halo(j, carry):
        arrived(pair_other + j)

        @pl.when(importer)
        def _():
            arrived(far_other + j)

        return carry

    pair_other = 2 * size * (1 - core)
    far_other = 2 * size * core
    lax.fori_loop(0, size, halo, 0)

    @pl.when(jnp.logical_not(importer))
    def _():
        ext[pl.ds(far_other, size)] = jnp.zeros((size, orb, lanes), ext.dtype)

    def ret_copy(i):
        return pltpu.make_async_remote_copy(
            src_ref=res.at[i],
            dst_ref=out_ref.at[0, loc],
            send_sem=ret_send.at[i],
            recv_sem=out_recv.at[loc],
            device_id=(grp, i),
            device_id_type=MESH,
        )

    def mix(q, carry):
        first = ((loc // run + q) % pieces) * chunk
        for m in range(modes):
            above = ext[pl.ds(size + first + shift_ref[m], chunk)]
            below = ext[pl.ds(size + first - shift_ref[m], chunk)]
            both = jnp.concatenate(
                [above.reshape(chunk * orb, lanes), below.reshape(chunk * orb, lanes)], 1
            )
            product = jnp.dot(both, right[m], preferred_element_type=jnp.float32)
            mid[:, m * orb : (m + 1) * orb] = product.astype(jnp.bfloat16).reshape(
                chunk, orb, lanes
            )
        finish(mid, res, first)
        for i in range(chunk):

            @pl.when(first + i != loc)
            def _():
                ret_copy(first + i).start()

        return carry

    lax.fori_loop(0, pieces, mix, 0)
    out_ref[0, loc] = res[loc]

    def settle(i, carry):
        @pl.when(i != loc)
        def _():
            pltpu.make_async_remote_copy(
                src_ref=res.at[i],
                dst_ref=out_ref.at[0, i],
                send_sem=ret_send.at[i],
                recv_sem=out_recv.at[i],
                device_id=(grp, i),
                device_id_type=MESH,
            ).wait()
            own_copy(i).wait_send()

        @pl.when(has_other & exports(i))
        def _():
            pltpu.make_async_remote_copy(
                src_ref=given.at[i],
                dst_ref=part.at[i],
                send_sem=give_send.at[i],
                recv_sem=part_recv.at[i],
                device_id=(other, i),
                device_id_type=MESH,
            ).wait_recv()
            total = out_ref[0, i].astype(jnp.float32) + part[i].astype(jnp.float32)
            out_ref[0, i] = total.astype(jnp.bfloat16)

            @pl.when(straight(loc, i))
            def _():
                far_copy(i).wait_send()

        @pl.when(exporter & jnp.logical_not(straight(i, loc)))
        def _():
            forward_copy(i).wait_send()

        @pl.when(importer)
        def _():
            give_copy(i).wait_send()

        pair_copy(i).wait_send()
        return carry

    lax.fori_loop(0, size, settle, 0)


def solution(mesh):
    groups = mesh.shape["egrp"]

    def step(green_blocks, sigma_prev, neighbours, couplings, occupancy, shifts):
        _, atoms, hops, orb, lanes = green_blocks.shape
        modes = couplings.shape[0]
        size = atoms
        vmem = pl.BlockSpec(memory_space=pltpu.VMEM)
        hbm = pl.BlockSpec(memory_space=pl.ANY)
        half = jnp.bfloat16
        return pl.pallas_call(
            functools.partial(kernel, groups),
            out_shape=pltpu.VMEM((1, atoms, orb, lanes), half),
            in_specs=[hbm] * 6,
            out_specs=vmem,
            scratch_shapes=[
                pltpu.SMEM(neighbours.shape[::-1], jnp.int32),
                pltpu.SMEM((modes,), jnp.float32),
                pltpu.SMEM((modes,), jnp.int32),
                pltpu.VMEM((atoms, hops, orb, lanes), half),
                pltpu.VMEM((atoms, orb, lanes), half),
                pltpu.VMEM(couplings.shape, half),
                pltpu.VMEM((atoms, lanes, lanes), half),
                pltpu.VMEM((atoms, orb, lanes), half),
                pltpu.VMEM((3 * size, orb, lanes), half),
                pltpu.VMEM((3 * size, orb, lanes), half),
                pltpu.VMEM((modes, 2 * lanes, lanes), half),
                pltpu.VMEM((lanes, modes * orb), half),
                pltpu.VMEM((4, modes * orb, lanes), half),
                pltpu.VMEM((size, orb, lanes), half),
                pltpu.VMEM((size, orb, lanes), half),
                pltpu.VMEM((size, orb, lanes), half),
                pltpu.SemaphoreType.DMA((atoms + 5,)),
                pltpu.SemaphoreType.DMA((size,)),
                pltpu.SemaphoreType.DMA((size,)),
                pltpu.SemaphoreType.DMA((size,)),
                pltpu.SemaphoreType.DMA((size,)),
                pltpu.SemaphoreType.DMA((size,)),
                pltpu.SemaphoreType.DMA((3 * size,)),
                pltpu.SemaphoreType.DMA((size,)),
                pltpu.SemaphoreType.DMA((size,)),
                pltpu.SemaphoreType.DMA((size,)),
                pltpu.SemaphoreType.REGULAR,
                pltpu.SemaphoreType.REGULAR,
            ],
            compiler_params=pltpu.CompilerParams(
                collective_id=0, has_side_effects=True
            ),
        )(neighbours.T, occupancy, shifts, green_blocks, sigma_prev, couplings)

    return jax.shard_map(
        step,
        mesh=mesh,
        in_specs=(
            P(("egrp", "eloc"), None, None, None, None),
            P(("egrp", "eloc"), None, None, None),
            P(),
            P(None, "eloc", None, None),
            P(),
            P(),
        ),
        out_specs=P(("egrp", "eloc"), None, None, None),
        check_vma=False,
    )
```

```python
import functools

import jax
import jax.numpy as jnp
from jax import lax
from jax.experimental import pallas as pl
from jax.experimental.pallas import tpu as pltpu
from jax.sharding import PartitionSpec as P

MESH = pl.DeviceIdType.MESH
RUN = 4


def signs(shape):
    half = shape[-1] // 2
    lane = lax.broadcasted_iota(jnp.int32, shape, len(shape) - 1)
    return jnp.where(lane < half, -1.0, 1.0).astype(jnp.float32)


def turned(block):
    wide = block.astype(jnp.float32)
    return pltpu.roll(wide, block.shape[-1] // 2, 1) * signs(block.shape)


def kernel(
    groups,
    near_hbm,
    occ_hbm,
    shift_hbm,
    green_hbm,
    sigma_hbm,
    coup_hbm,
    out_ref,
    near_ref,
    occ_ref,
    shift_ref,
    green,
    sigma,
    coup_ref,
    wide,
    mine,
    own,
    ext,
    right,
    left,
    mid,
    res,
    given,
    part,
    in_sem,
    own_send,
    far_send,
    fwd_send,
    pair_send,
    ret_send,
    ext_recv,
    out_recv,
    give_send,
    part_recv,
    far_sem,
    all_sem,
):
    atoms, orb, lanes = sigma.shape
    size = atoms
    modes = right.shape[0]
    chunk = 4
    batch = min(4, size // 2)
    lag = batch
    run = min(RUN, size // 2)
    grp = lax.axis_index("egrp")
    loc = lax.axis_index("eloc")
    core = grp % 2
    partner = grp + 1 - 2 * core
    other = grp - 1 + 2 * core
    has_other = (other >= 0) & (other < groups)
    here = loc % run

    pieces = atoms // chunk

    def turn(t):
        return (loc + t) % size

    def load_green(t):
        return pltpu.make_async_copy(
            green_hbm.at[0, turn(t)], green.at[turn(t)], in_sem.at[t - 1]
        )

    load_near = pltpu.make_async_copy(near_hbm, near_ref, in_sem.at[atoms])
    load_sigma = pltpu.make_async_copy(sigma_hbm.at[0], sigma, in_sem.at[atoms + 1])
    load_occ = pltpu.make_async_copy(occ_hbm, occ_ref, in_sem.at[atoms + 2])
    load_shift = pltpu.make_async_copy(shift_hbm, shift_ref, in_sem.at[atoms + 3])
    load_coup = pltpu.make_async_copy(coup_hbm, coup_ref, in_sem.at[atoms + 4])
    load_sigma.start()
    load_near.start()

    def fetch(t, carry):
        load_green(t).start()
        return carry

    lax.fori_loop(1, size + 1, fetch, 0)
    load_coup.start()
    load_occ.start()
    load_shift.start()

    def straight(source, worker):
        rise = source % run - worker % run
        return rise * (2 * core - 1) > 0

    def exports(worker):
        return worker % run // (run // 2) != core

    exporter = has_other & exports(loc)
    importer = has_other & jnp.logical_not(exports(loc))

    def reaches(i):
        return straight(loc, i) | (i == loc)

    hi = (grp // 2) % 4
    lead = jnp.where(core == 1, jnp.where(hi == 3, 0, 1), jnp.where(hi == 0, 1, 0))
    nearer = (core * here + (1 - core) * (run - 1 - here)) * (size // run)
    barrier = pltpu.get_barrier_semaphore()

    def greet(i, carry):
        @pl.when(i != loc)
        def _():
            pl.semaphore_signal(
                barrier, inc=1, device_id=(grp, i), device_id_type=MESH
            )

        @pl.when(has_other & (lead == 1) & reaches(i))
        def _():
            pl.semaphore_signal(
                barrier, inc=1, device_id=(other, i), device_id_type=MESH
            )

        return carry

    lax.fori_loop(0, size, greet, 0)
    pl.semaphore_signal(
        barrier, inc=1, device_id=(partner, loc), device_id_type=MESH
    )

    own[pl.ds(0, size)] = jnp.zeros((size, orb, lanes), own.dtype)
    own[pl.ds(2 * size, size)] = jnp.zeros((size, orb, lanes), own.dtype)
    load_near.wait()
    load_sigma.wait()

    def widen(n, carry):
        block = sigma[n]
        wide[n, :orb] = block
        wide[n, orb:] = turned(block).astype(jnp.bfloat16)
        return carry

    lax.fori_loop(0, atoms, widen, 0, unroll=2)

    def lesser(start):
        for t in range(batch):
            load_green(start + t).wait()
        halves = []
        for t in range(batch):
            a = turn(start + t)
            row = []
            for k in range(3):
                n = a if k == 0 else near_ref[k - 1, a]
                row.append(
                    jnp.dot(
                        green[a, k], wide[n], preferred_element_type=jnp.float32
                    ).astype(jnp.bfloat16)
                )
            halves.append(jnp.concatenate(row, 1))
        for t in range(batch):
            a = turn(start + t)
            upper = jnp.concatenate([green[a, k] for k in range(3)], 1)
            lower = jnp.concatenate(
                [turned(green[a, k]).astype(jnp.bfloat16) for k in range(3)], 1
            )
            form = jnp.concatenate([upper, lower], 0)
            mine[a] = lax.dot_general(
                halves[t],
                form,
                (((1,), (1,)), ((), ())),
                preferred_element_type=jnp.float32,
            ).astype(jnp.bfloat16)

    def first(t, carry):
        lesser(batch * t + 1)
        return carry

    lax.fori_loop(0, lag // batch, first, 0)

    load_coup.wait()
    load_occ.wait()
    load_shift.wait()
    for m in range(modes):
        block = coup_ref[m, 0].astype(jnp.float32)
        adjoint = jnp.concatenate([block, turned(coup_ref[m, 0])], 0).T
        right[m, :lanes] = (adjoint * (occ_ref[m] + 1.0)).astype(jnp.bfloat16)
        right[m, lanes:] = (adjoint * occ_ref[m]).astype(jnp.bfloat16)
    low = lax.broadcasted_iota(jnp.int32, (orb, lanes), 1) < orb
    for m in range(0, modes, 2):
        one = coup_ref[m, 0].astype(jnp.float32)
        two = coup_ref[m + 1, 0].astype(jnp.float32)
        span = slice(m * orb, m * orb + lanes)
        left[:orb, span] = jnp.where(low, one, pltpu.roll(two, orb, 1)).astype(
            jnp.bfloat16
        )
        left[orb:, span] = jnp.where(low, pltpu.roll(one, orb, 1), two).astype(
            jnp.bfloat16
        )

    @pl.when(has_other & (lead == 0))
    def _():
        pl.semaphore_wait(barrier, size + 1 + nearer)

        def answer(i, carry):
            @pl.when(reaches(i))
            def _():
                pl.semaphore_signal(
                    far_sem, inc=1, device_id=(other, i), device_id_type=MESH
                )

            return carry

        lax.fori_loop(0, size, answer, 0)

    @pl.when(jnp.logical_not(has_other & (lead == 0)))
    def _():
        pl.semaphore_wait(barrier, size)

    far_base = 2 * size * (1 - core)
    pair_base = 2 * size * core

    def own_copy(a):
        return pltpu.make_async_remote_copy(
            src_ref=mine.at[a],
            dst_ref=own.at[size + loc],
            send_sem=own_send.at[a],
            recv_sem=ext_recv.at[size + loc],
            device_id=(grp, a),
            device_id_type=MESH,
        )

    def far_copy(a):
        return pltpu.make_async_remote_copy(
            src_ref=mine.at[a],
            dst_ref=ext.at[far_base + loc],
            send_sem=far_send.at[a],
            recv_sem=ext_recv.at[far_base + loc],
            device_id=(other, a),
            device_id_type=MESH,
        )

    def forward_copy(j):
        return pltpu.make_async_remote_copy(
            src_ref=own.at[size + j],
            dst_ref=ext.at[far_base + j],
            send_sem=fwd_send.at[j],
            recv_sem=ext_recv.at[far_base + j],
            device_id=(other, loc),
            device_id_type=MESH,
        )

    def pair_copy(j):
        return pltpu.make_async_remote_copy(
            src_ref=own.at[size + j],
            dst_ref=ext.at[pair_base + j],
            send_sem=pair_send.at[j],
            recv_sem=ext_recv.at[pair_base + j],
            device_id=(partner, loc),
            device_id_type=MESH,
        )

    def arrived(slot):
        pltpu.make_async_remote_copy(
            src_ref=ext.at[slot],
            dst_ref=ext.at[slot],
            send_sem=own_send.at[0],
            recv_sem=ext_recv.at[slot],
            device_id=(partner, loc),
            device_id_type=MESH,
        ).wait_recv()

    def send(t):
        a = turn(t)

        own_copy(a).start()

    def later(t, carry):
        for i in range(batch):
            send(batch * t + 1 - lag + i)
        lesser(batch * t + 1)
        return carry

    def last(t, carry):
        send(t)
        return carry

    lax.fori_loop(lag // batch, size // batch, later, 0)
    lax.fori_loop(size - lag + 1, size, last, 0)
    own[size + loc] = mine[loc]

    def direct(t, carry):
        @pl.when(straight(loc, turn(t)) & exports(turn(t)))
        def _():
            far_copy(turn(t)).start()

        return carry

    @pl.when(has_other & (lead == 0))
    def _():
        lax.fori_loop(1, size, direct, 0)

    def source(t):
        return (loc + size - t) % size

    def forward(t):
        @pl.when(exporter & jnp.logical_not(straight(source(t), loc)))
        def _():
            forward_copy(source(t)).start()

    def early(t, carry):
        @pl.when(t > 0)
        def _():
            arrived(size + source(t))

        @pl.when(lead == 0)
        def _():
            forward(t)

        pair_copy(source(t)).start()
        return carry

    def late(t, carry):
        arrived(size + source(t))
        forward(t)
        pair_copy(source(t)).start()
        return carry

    lax.fori_loop(0, size // 4, early, 0)

    @pl.when(has_other & (lead == 1))
    def _():
        pl.semaphore_wait(far_sem, 1 + nearer)
        pl.semaphore_signal(
            all_sem, inc=1, device_id=(other, loc), device_id_type=MESH
        )

        def delayed(t, carry):
            forward(t)
            return carry

        lax.fori_loop(1, size, direct, 0)
        lax.fori_loop(0, size // 4, delayed, 0)

    lax.fori_loop(size // 4, size, late, 0)

    ext[pl.ds(size, size)] = own[pl.ds(size, size)]

    @pl.when(has_other & (lead == 0))
    def _():
        pl.semaphore_wait(all_sem, 1)

    def give_copy(i):
        return pltpu.make_async_remote_copy(
            src_ref=given.at[i],
            dst_ref=part.at[loc],
            send_sem=give_send.at[i],
            recv_sem=part_recv.at[loc],
            device_id=(other, i),
            device_id_type=MESH,
        )

    def finish(m_blocks, target, first):
        for i in range(chunk):
            parts = jnp.dot(left[...], m_blocks[i], preferred_element_type=jnp.float32)
            value = parts[:orb] + pltpu.roll(parts[orb:], orb, 1) * signs((orb, lanes))
            target[first + i] = value.astype(jnp.bfloat16)

    @pl.when(importer)
    def _():
        def give(q, carry):
            first = ((loc // run + q) % pieces) * chunk
            for m in range(modes):
                start = first + shift_ref[m] + core * (2 * size - 2 * shift_ref[m])
                block = own[pl.ds(start, chunk)].reshape(chunk * orb, lanes)
                product = jnp.dot(
                    block,
                    right[m, pl.ds(core * lanes, lanes)],
                    preferred_element_type=jnp.float32,
                )
                mid[:, m * orb : (m + 1) * orb] = product.astype(
                    jnp.bfloat16
                ).reshape(chunk, orb, lanes)
            finish(mid, given, first)
            for i in range(chunk):
                give_copy(first + i).start()
            return carry

        lax.fori_loop(0, pieces, give, 0)

    def halo(j, carry):
        arrived(pair_other + j)

        @pl.when(importer)
        def _():
            arrived(far_other + j)

        return carry

    pair_other = 2 * size * (1 - core)
    far_other = 2 * size * core
    lax.fori_loop(0, size, halo, 0)

    @pl.when(jnp.logical_not(importer))
    def _():
        ext[pl.ds(far_other, size)] = jnp.zeros((size, orb, lanes), ext.dtype)

    def ret_copy(i):
        return pltpu.make_async_remote_copy(
            src_ref=res.at[i],
            dst_ref=out_ref.at[0, loc],
            send_sem=ret_send.at[i],
            recv_sem=out_recv.at[loc],
            device_id=(grp, i),
            device_id_type=MESH,
        )

    def mix(q, carry):
        first = ((loc // run + q) % pieces) * chunk
        for m in range(modes):
            above = ext[pl.ds(size + first + shift_ref[m], chunk)]
            below = ext[pl.ds(size + first - shift_ref[m], chunk)]
            both = jnp.concatenate(
                [above.reshape(chunk * orb, lanes), below.reshape(chunk * orb, lanes)], 1
            )
            product = jnp.dot(both, right[m], preferred_element_type=jnp.float32)
            mid[:, m * orb : (m + 1) * orb] = product.astype(jnp.bfloat16).reshape(
                chunk, orb, lanes
            )
        finish(mid, res, first)
        for i in range(chunk):

            @pl.when(first + i != loc)
            def _():
                ret_copy(first + i).start()

        return carry

    lax.fori_loop(0, pieces, mix, 0)
    out_ref[0, loc] = res[loc]

    def sent(i, carry):
        @pl.when(i != loc)
        def _():
            own_copy(i).wait_send()
            ret_copy(i).wait_send()

        @pl.when(has_other & exports(i) & straight(loc, i))
        def _():
            far_copy(i).wait_send()

        @pl.when(exporter & jnp.logical_not(straight(i, loc)))
        def _():
            forward_copy(i).wait_send()

        @pl.when(importer)
        def _():
            give_copy(i).wait_send()

        pair_copy(i).wait_send()
        return carry

    lax.fori_loop(0, size, sent, 0)

    def settle(t, carry):
        i = turn(t)

        @pl.when(t > 0)
        def _():
            pltpu.make_async_remote_copy(
                src_ref=res.at[i],
                dst_ref=out_ref.at[0, i],
                send_sem=ret_send.at[i],
                recv_sem=out_recv.at[i],
                device_id=(partner, loc),
                device_id_type=MESH,
            ).wait_recv()

        @pl.when(has_other & exports(i))
        def _():
            pltpu.make_async_remote_copy(
                src_ref=given.at[i],
                dst_ref=part.at[i],
                send_sem=give_send.at[i],
                recv_sem=part_recv.at[i],
                device_id=(partner, loc),
                device_id_type=MESH,
            ).wait_recv()
            total = out_ref[0, i].astype(jnp.float32) + part[i].astype(jnp.float32)
            out_ref[0, i] = total.astype(jnp.bfloat16)

        return carry

    lax.fori_loop(0, size, settle, 0)


def solution(mesh):
    groups = mesh.shape["egrp"]

    def step(green_blocks, sigma_prev, neighbours, couplings, occupancy, shifts):
        _, atoms, hops, orb, lanes = green_blocks.shape
        modes = couplings.shape[0]
        size = atoms
        vmem = pl.BlockSpec(memory_space=pltpu.VMEM)
        hbm = pl.BlockSpec(memory_space=pl.ANY)
        half = jnp.bfloat16
        return pl.pallas_call(
            functools.partial(kernel, groups),
            out_shape=pltpu.VMEM((1, atoms, orb, lanes), half),
            in_specs=[hbm] * 6,
            out_specs=vmem,
            scratch_shapes=[
                pltpu.SMEM(neighbours.shape[::-1], jnp.int32),
                pltpu.SMEM((modes,), jnp.float32),
                pltpu.SMEM((modes,), jnp.int32),
                pltpu.VMEM((atoms, hops, orb, lanes), half),
                pltpu.VMEM((atoms, orb, lanes), half),
                pltpu.VMEM(couplings.shape, half),
                pltpu.VMEM((atoms, lanes, lanes), half),
                pltpu.VMEM((atoms, orb, lanes), half),
                pltpu.VMEM((3 * size, orb, lanes), half),
                pltpu.VMEM((3 * size, orb, lanes), half),
                pltpu.VMEM((modes, 2 * lanes, lanes), half),
                pltpu.VMEM((lanes, modes * orb), half),
                pltpu.VMEM((4, modes * orb, lanes), half),
                pltpu.VMEM((size, orb, lanes), half),
                pltpu.VMEM((size, orb, lanes), half),
                pltpu.VMEM((size, orb, lanes), half),
                pltpu.SemaphoreType.DMA((atoms + 5,)),
                pltpu.SemaphoreType.DMA((size,)),
                pltpu.SemaphoreType.DMA((size,)),
                pltpu.SemaphoreType.DMA((size,)),
                pltpu.SemaphoreType.DMA((size,)),
                pltpu.SemaphoreType.DMA((size,)),
                pltpu.SemaphoreType.DMA((3 * size,)),
                pltpu.SemaphoreType.DMA((size,)),
                pltpu.SemaphoreType.DMA((size,)),
                pltpu.SemaphoreType.DMA((size,)),
                pltpu.SemaphoreType.REGULAR,
                pltpu.SemaphoreType.REGULAR,
            ],
            compiler_params=pltpu.CompilerParams(
                collective_id=0, has_side_effects=True
            ),
        )(neighbours.T, occupancy, shifts, green_blocks, sigma_prev, couplings)

    return jax.shard_map(
        step,
        mesh=mesh,
        in_specs=(
            P(("egrp", "eloc"), None, None, None, None),
            P(("egrp", "eloc"), None, None, None),
            P(),
            P(None, "eloc", None, None),
            P(),
            P(),
        ),
        out_specs=P(("egrp", "eloc"), None, None, None),
        check_vma=False,
    )
```

```python
import functools

import jax
import jax.numpy as jnp
from jax import lax
from jax.experimental import pallas as pl
from jax.experimental.pallas import tpu as pltpu
from jax.sharding import PartitionSpec as P

MESH = pl.DeviceIdType.MESH
RUN = 4


def signs(shape):
    half = shape[-1] // 2
    lane = lax.broadcasted_iota(jnp.int32, shape, len(shape) - 1)
    return jnp.where(lane < half, -1.0, 1.0).astype(jnp.float32)


def turned(block):
    wide = block.astype(jnp.float32)
    return pltpu.roll(wide, block.shape[-1] // 2, 1) * signs(block.shape)


def kernel(
    groups,
    near_hbm,
    occ_hbm,
    shift_hbm,
    green_hbm,
    sigma_hbm,
    coup_hbm,
    out_ref,
    near_ref,
    occ_ref,
    shift_ref,
    green,
    sigma,
    coup_ref,
    wide,
    mine,
    own,
    ext,
    right,
    left,
    mid,
    res,
    given,
    part,
    in_sem,
    own_send,
    far_send,
    pair_send,
    ret_send,
    ext_recv,
    out_recv,
    give_send,
    part_recv,
    far_sem,
):
    atoms, orb, lanes = sigma.shape
    size = atoms
    modes = right.shape[0]
    chunk = mid.shape[0]
    batch = min(4, size // 2)
    lag = batch
    run = min(RUN, size // 2)
    grp = lax.axis_index("egrp")
    loc = lax.axis_index("eloc")
    core = grp % 2
    partner = grp + 1 - 2 * core
    other = grp - 1 + 2 * core
    has_other = (other >= 0) & (other < groups)
    here = loc % run

    pieces = atoms // chunk

    def turn(t):
        return (loc + t) % size

    def load_green(t):
        return pltpu.make_async_copy(
            green_hbm.at[0, turn(t)], green.at[turn(t)], in_sem.at[t - 1]
        )

    load_near = pltpu.make_async_copy(near_hbm, near_ref, in_sem.at[atoms])
    load_sigma = pltpu.make_async_copy(sigma_hbm.at[0], sigma, in_sem.at[atoms + 1])
    load_occ = pltpu.make_async_copy(occ_hbm, occ_ref, in_sem.at[atoms + 2])
    load_shift = pltpu.make_async_copy(shift_hbm, shift_ref, in_sem.at[atoms + 3])
    load_coup = pltpu.make_async_copy(coup_hbm, coup_ref, in_sem.at[atoms + 4])
    load_sigma.start()
    load_near.start()

    def fetch(t, carry):
        load_green(t).start()
        return carry

    lax.fori_loop(1, size + 1, fetch, 0)
    load_coup.start()
    load_occ.start()
    load_shift.start()

    def exports(worker):
        return worker % run // (run // 2) != core

    importer = has_other & jnp.logical_not(exports(loc))

    hi = (grp // 2) % 4
    lead = jnp.where(core == 1, jnp.where(hi == 3, 0, 1), jnp.where(hi == 0, 1, 0))
    barrier = pltpu.get_barrier_semaphore()

    def greet(i, carry):
        @pl.when(i != loc)
        def _():
            pl.semaphore_signal(
                barrier, inc=1, device_id=(grp, i), device_id_type=MESH
            )

        @pl.when(has_other & (lead == 1))
        def _():
            pl.semaphore_signal(
                barrier, inc=1, device_id=(other, i), device_id_type=MESH
            )

        return carry

    lax.fori_loop(0, size, greet, 0)
    pl.semaphore_signal(
        barrier, inc=1, device_id=(partner, loc), device_id_type=MESH
    )

    own[pl.ds(0, size)] = jnp.zeros((size, orb, lanes), own.dtype)
    own[pl.ds(2 * size, size)] = jnp.zeros((size, orb, lanes), own.dtype)
    load_near.wait()
    load_sigma.wait()

    def widen(n, carry):
        block = sigma[n]
        wide[n, :orb] = block
        wide[n, orb:] = turned(block).astype(jnp.bfloat16)
        return carry

    lax.fori_loop(0, atoms, widen, 0, unroll=2)

    def lesser(start):
        for t in range(batch):
            load_green(start + t).wait()
        halves = []
        for t in range(batch):
            a = turn(start + t)
            row = []
            for k in range(3):
                n = a if k == 0 else near_ref[k - 1, a]
                row.append(
                    jnp.dot(
                        green[a, k], wide[n], preferred_element_type=jnp.float32
                    ).astype(jnp.bfloat16)
                )
            halves.append(jnp.concatenate(row, 1))
        for t in range(batch):
            a = turn(start + t)
            upper = jnp.concatenate([green[a, k] for k in range(3)], 1)
            lower = jnp.concatenate(
                [turned(green[a, k]).astype(jnp.bfloat16) for k in range(3)], 1
            )
            form = jnp.concatenate([upper, lower], 0)
            mine[a] = lax.dot_general(
                halves[t],
                form,
                (((1,), (1,)), ((), ())),
                preferred_element_type=jnp.float32,
            ).astype(jnp.bfloat16)

    def first(t, carry):
        lesser(batch * t + 1)
        return carry

    lax.fori_loop(0, lag // batch, first, 0)

    load_coup.wait()
    load_occ.wait()
    load_shift.wait()
    for m in range(modes):
        block = coup_ref[m, 0].astype(jnp.float32)
        adjoint = jnp.concatenate([block, turned(coup_ref[m, 0])], 0).T
        right[m, :lanes] = (adjoint * (occ_ref[m] + 1.0)).astype(jnp.bfloat16)
        right[m, lanes:] = (adjoint * occ_ref[m]).astype(jnp.bfloat16)
    low = lax.broadcasted_iota(jnp.int32, (orb, lanes), 1) < orb
    for m in range(0, modes, 2):
        one = coup_ref[m, 0].astype(jnp.float32)
        two = coup_ref[m + 1, 0].astype(jnp.float32)
        span = slice(m * orb, m * orb + lanes)
        left[:orb, span] = jnp.where(low, one, pltpu.roll(two, orb, 1)).astype(
            jnp.bfloat16
        )
        left[orb:, span] = jnp.where(low, pltpu.roll(one, orb, 1), two).astype(
            jnp.bfloat16
        )

    @pl.when(has_other & (lead == 0))
    def _():
        pl.semaphore_wait(barrier, 2 * size)

        def answer(i, carry):
            pl.semaphore_signal(
                far_sem, inc=1, device_id=(other, i), device_id_type=MESH
            )
            return carry

        lax.fori_loop(0, size, answer, 0)

    @pl.when(jnp.logical_not(has_other & (lead == 0)))
    def _():
        pl.semaphore_wait(barrier, size)

    far_base = 2 * size * (1 - core)
    pair_base = 2 * size * core

    def own_copy(a):
        return pltpu.make_async_remote_copy(
            src_ref=mine.at[a],
            dst_ref=own.at[size + loc],
            send_sem=own_send.at[a],
            recv_sem=ext_recv.at[size + loc],
            device_id=(grp, a),
            device_id_type=MESH,
        )

    def far_copy(a):
        return pltpu.make_async_remote_copy(
            src_ref=mine.at[a],
            dst_ref=ext.at[far_base + loc],
            send_sem=far_send.at[a],
            recv_sem=ext_recv.at[far_base + loc],
            device_id=(other, a),
            device_id_type=MESH,
        )

    def pair_copy(j):
        return pltpu.make_async_remote_copy(
            src_ref=own.at[size + j],
            dst_ref=ext.at[pair_base + j],
            send_sem=pair_send.at[j],
            recv_sem=ext_recv.at[pair_base + j],
            device_id=(partner, loc),
            device_id_type=MESH,
        )

    def arrived(slot):
        pltpu.make_async_remote_copy(
            src_ref=ext.at[slot],
            dst_ref=ext.at[slot],
            send_sem=own_send.at[0],
            recv_sem=ext_recv.at[slot],
            device_id=(partner, loc),
            device_id_type=MESH,
        ).wait_recv()

    def send(t):
        a = turn(t)

        own_copy(a).start()

    def later(t, carry):
        for i in range(batch):
            send(batch * t + 1 - lag + i)
        lesser(batch * t + 1)
        return carry

    def last(t, carry):
        send(t)
        return carry

    lax.fori_loop(lag // batch, size // batch, later, 0)
    lax.fori_loop(size - lag + 1, size, last, 0)
    own[size + loc] = mine[loc]

    def direct(t, carry):
        @pl.when(exports(turn(t)))
        def _():
            far_copy(turn(t)).start()

        return carry

    @pl.when(has_other & (lead == 0))
    def _():
        lax.fori_loop(1, size + 1, direct, 0)

    def source(t):
        return (loc + size - t) % size

    def early(t, carry):
        @pl.when(t > 0)
        def _():
            arrived(size + source(t))

        pair_copy(source(t)).start()
        return carry

    def late(t, carry):
        arrived(size + source(t))
        pair_copy(source(t)).start()
        return carry

    lax.fori_loop(0, size - size // 4, early, 0)

    @pl.when(has_other & (lead == 1))
    def _():
        pl.semaphore_wait(far_sem, size)

        lax.fori_loop(1, size + 1, direct, 0)

    lax.fori_loop(size - size // 4, size, late, 0)

    ext[pl.ds(size, size)] = own[pl.ds(size, size)]

    def give_copy(i):
        return pltpu.make_async_remote_copy(
            src_ref=given.at[i],
            dst_ref=part.at[loc],
            send_sem=give_send.at[i],
            recv_sem=part_recv.at[loc],
            device_id=(other, i),
            device_id_type=MESH,
        )

    def finish(m_blocks, target, first):
        for i in range(chunk):
            parts = jnp.dot(left[...], m_blocks[i], preferred_element_type=jnp.float32)
            value = parts[:orb] + pltpu.roll(parts[orb:], orb, 1) * signs((orb, lanes))
            target[first + i] = value.astype(jnp.bfloat16)

    @pl.when(importer)
    def _():
        def give(q, carry):
            first = ((loc // run + q) % pieces) * chunk
            for m in range(modes):
                start = first + shift_ref[m] + core * (2 * size - 2 * shift_ref[m])
                block = own[pl.ds(start, chunk)].reshape(chunk * orb, lanes)
                product = jnp.dot(
                    block,
                    right[m, pl.ds(core * lanes, lanes)],
                    preferred_element_type=jnp.float32,
                )
                mid[:, m * orb : (m + 1) * orb] = product.astype(
                    jnp.bfloat16
                ).reshape(chunk, orb, lanes)
            finish(mid, given, first)
            for i in range(chunk):
                give_copy(first + i).start()
            return carry

        lax.fori_loop(0, pieces, give, 0)

    def halo(j, carry):
        arrived(pair_other + j)

        @pl.when(importer)
        def _():
            arrived(far_other + j)

        return carry

    pair_other = 2 * size * (1 - core)
    far_other = 2 * size * core
    lax.fori_loop(0, size, halo, 0)

    @pl.when(jnp.logical_not(importer))
    def _():
        ext[pl.ds(far_other, size)] = jnp.zeros((size, orb, lanes), ext.dtype)

    def ret_copy(i):
        return pltpu.make_async_remote_copy(
            src_ref=res.at[i],
            dst_ref=out_ref.at[0, loc],
            send_sem=ret_send.at[i],
            recv_sem=out_recv.at[loc],
            device_id=(grp, i),
            device_id_type=MESH,
        )

    def mix(q, carry):
        first = ((loc // run + q) % pieces) * chunk
        for m in range(modes):
            above = ext[pl.ds(size + first + shift_ref[m], chunk)]
            below = ext[pl.ds(size + first - shift_ref[m], chunk)]
            both = jnp.concatenate(
                [above.reshape(chunk * orb, lanes), below.reshape(chunk * orb, lanes)], 1
            )
            product = jnp.dot(both, right[m], preferred_element_type=jnp.float32)
            mid[:, m * orb : (m + 1) * orb] = product.astype(jnp.bfloat16).reshape(
                chunk, orb, lanes
            )
        finish(mid, res, first)
        for i in range(chunk):

            @pl.when(first + i != loc)
            def _():
                ret_copy(first + i).start()

        return carry

    lax.fori_loop(0, pieces, mix, 0)
    out_ref[0, loc] = res[loc]

    def sent(i, carry):
        @pl.when(i != loc)
        def _():
            own_copy(i).wait_send()
            ret_copy(i).wait_send()

        @pl.when(has_other & exports(i))
        def _():
            far_copy(i).wait_send()

        @pl.when(importer)
        def _():
            give_copy(i).wait_send()

        pair_copy(i).wait_send()
        return carry

    lax.fori_loop(0, size, sent, 0)

    def settle(t, carry):
        i = turn(t)

        @pl.when(t > 0)
        def _():
            pltpu.make_async_remote_copy(
                src_ref=res.at[i],
                dst_ref=out_ref.at[0, i],
                send_sem=ret_send.at[i],
                recv_sem=out_recv.at[i],
                device_id=(partner, loc),
                device_id_type=MESH,
            ).wait_recv()

        @pl.when(has_other & exports(i))
        def _():
            pltpu.make_async_remote_copy(
                src_ref=given.at[i],
                dst_ref=part.at[i],
                send_sem=give_send.at[i],
                recv_sem=part_recv.at[i],
                device_id=(partner, loc),
                device_id_type=MESH,
            ).wait_recv()
            total = out_ref[0, i].astype(jnp.float32) + part[i].astype(jnp.float32)
            out_ref[0, i] = total.astype(jnp.bfloat16)

        return carry

    lax.fori_loop(0, size, settle, 0)


def solution(mesh):
    groups = mesh.shape["egrp"]

    def step(green_blocks, sigma_prev, neighbours, couplings, occupancy, shifts):
        _, atoms, hops, orb, lanes = green_blocks.shape
        modes = couplings.shape[0]
        size = atoms
        vmem = pl.BlockSpec(memory_space=pltpu.VMEM)
        hbm = pl.BlockSpec(memory_space=pl.ANY)
        half = jnp.bfloat16
        return pl.pallas_call(
            functools.partial(kernel, groups),
            out_shape=pltpu.VMEM((1, atoms, orb, lanes), half),
            in_specs=[hbm] * 6,
            out_specs=vmem,
            scratch_shapes=[
                pltpu.SMEM(neighbours.shape[::-1], jnp.int32),
                pltpu.SMEM((modes,), jnp.float32),
                pltpu.SMEM((modes,), jnp.int32),
                pltpu.VMEM((atoms, hops, orb, lanes), half),
                pltpu.VMEM((atoms, orb, lanes), half),
                pltpu.VMEM(couplings.shape, half),
                pltpu.VMEM((atoms, lanes, lanes), half),
                pltpu.VMEM((atoms, orb, lanes), half),
                pltpu.VMEM((3 * size, orb, lanes), half),
                pltpu.VMEM((3 * size, orb, lanes), half),
                pltpu.VMEM((modes, 2 * lanes, lanes), half),
                pltpu.VMEM((lanes, modes * orb), half),
                pltpu.VMEM((min(8, size // 2), modes * orb, lanes), half),
                pltpu.VMEM((size, orb, lanes), half),
                pltpu.VMEM((size, orb, lanes), half),
                pltpu.VMEM((size, orb, lanes), half),
                pltpu.SemaphoreType.DMA((atoms + 5,)),
                pltpu.SemaphoreType.DMA((size,)),
                pltpu.SemaphoreType.DMA((size,)),
                pltpu.SemaphoreType.DMA((size,)),
                pltpu.SemaphoreType.DMA((size,)),
                pltpu.SemaphoreType.DMA((3 * size,)),
                pltpu.SemaphoreType.DMA((size,)),
                pltpu.SemaphoreType.DMA((size,)),
                pltpu.SemaphoreType.DMA((size,)),
                pltpu.SemaphoreType.REGULAR,
            ],
            compiler_params=pltpu.CompilerParams(
                collective_id=0, has_side_effects=True
            ),
        )(neighbours.T, occupancy, shifts, green_blocks, sigma_prev, couplings)

    return jax.shard_map(
        step,
        mesh=mesh,
        in_specs=(
            P(("egrp", "eloc"), None, None, None, None),
            P(("egrp", "eloc"), None, None, None),
            P(),
            P(None, "eloc", None, None),
            P(),
            P(),
        ),
        out_specs=P(("egrp", "eloc"), None, None, None),
        check_vma=False,
    )
```

```python
import functools

import jax
import jax.numpy as jnp
from jax import lax
from jax.experimental import pallas as pl
from jax.experimental.pallas import tpu as pltpu
from jax.sharding import PartitionSpec as P

MESH = pl.DeviceIdType.MESH
RUN = 4


def signs(shape):
    half = shape[-1] // 2
    lane = lax.broadcasted_iota(jnp.int32, shape, len(shape) - 1)
    return jnp.where(lane < half, -1.0, 1.0).astype(jnp.float32)


def turned(block):
    wide = block.astype(jnp.float32)
    return pltpu.roll(wide, block.shape[-1] // 2, 1) * signs(block.shape)


def kernel(
    groups,
    near_hbm,
    occ_hbm,
    shift_hbm,
    green_hbm,
    sigma_hbm,
    coup_hbm,
    out_ref,
    near_ref,
    occ_ref,
    shift_ref,
    green,
    sigma,
    coup_ref,
    wide,
    mine,
    own,
    ext,
    right,
    left,
    mid,
    res,
    given,
    part,
    in_sem,
    own_send,
    far_send,
    pair_send,
    ret_send,
    ext_recv,
    out_recv,
    give_send,
    part_recv,
    far_sem,
):
    atoms, orb, lanes = sigma.shape
    size = atoms
    modes = right.shape[0]
    chunk = mid.shape[0]
    batch = min(4, size // 2)
    lag = batch
    run = min(RUN, size // 2)
    grp = lax.axis_index("egrp")
    loc = lax.axis_index("eloc")
    core = grp % 2
    partner = grp + 1 - 2 * core
    other = grp - 1 + 2 * core
    has_other = (other >= 0) & (other < groups)
    here = loc % run

    pieces = atoms // chunk

    def turn(t):
        return (loc + t) % size

    def load_green(t):
        return pltpu.make_async_copy(
            green_hbm.at[0, turn(t)], green.at[turn(t)], in_sem.at[t - 1]
        )

    load_near = pltpu.make_async_copy(near_hbm, near_ref, in_sem.at[atoms])
    load_sigma = pltpu.make_async_copy(sigma_hbm.at[0], sigma, in_sem.at[atoms + 1])
    load_occ = pltpu.make_async_copy(occ_hbm, occ_ref, in_sem.at[atoms + 2])
    load_shift = pltpu.make_async_copy(shift_hbm, shift_ref, in_sem.at[atoms + 3])
    load_coup = pltpu.make_async_copy(coup_hbm, coup_ref, in_sem.at[atoms + 4])
    def exports(worker):
        return worker % run // (run // 2) != core

    importer = has_other & jnp.logical_not(exports(loc))

    hi = (grp // 2) % 4
    lead = jnp.where(core == 1, jnp.where(hi == 3, 0, 1), jnp.where(hi == 0, 1, 0))
    barrier = pltpu.get_barrier_semaphore()

    def greet(i, carry):
        @pl.when(i != loc)
        def _():
            pl.semaphore_signal(
                barrier, inc=1, device_id=(grp, i), device_id_type=MESH
            )

        @pl.when(has_other & (lead == 1))
        def _():
            pl.semaphore_signal(
                barrier, inc=1, device_id=(other, i), device_id_type=MESH
            )

        return carry

    lax.fori_loop(0, size, greet, 0)
    pl.semaphore_signal(
        barrier, inc=1, device_id=(partner, loc), device_id_type=MESH
    )

    load_sigma.start()
    load_near.start()

    def fetch(t, carry):
        load_green(t).start()
        return carry

    lax.fori_loop(1, size + 1, fetch, 0)
    load_coup.start()
    load_occ.start()
    load_shift.start()

    own[pl.ds(0, size)] = jnp.zeros((size, orb, lanes), own.dtype)
    own[pl.ds(2 * size, size)] = jnp.zeros((size, orb, lanes), own.dtype)
    load_near.wait()
    load_sigma.wait()

    def widen(n, carry):
        block = sigma[n]
        wide[n, :orb] = block
        wide[n, orb:] = turned(block).astype(jnp.bfloat16)
        return carry

    lax.fori_loop(0, atoms, widen, 0, unroll=2)

    def lesser(start):
        for t in range(batch):
            load_green(start + t).wait()
        halves = []
        for t in range(batch):
            a = turn(start + t)
            row = []
            for k in range(3):
                n = a if k == 0 else near_ref[k - 1, a]
                row.append(
                    jnp.dot(
                        green[a, k], wide[n], preferred_element_type=jnp.float32
                    ).astype(jnp.bfloat16)
                )
            halves.append(jnp.concatenate(row, 1))
        for t in range(batch):
            a = turn(start + t)
            upper = jnp.concatenate([green[a, k] for k in range(3)], 1)
            lower = jnp.concatenate(
                [turned(green[a, k]).astype(jnp.bfloat16) for k in range(3)], 1
            )
            form = jnp.concatenate([upper, lower], 0)
            mine[a] = lax.dot_general(
                halves[t],
                form,
                (((1,), (1,)), ((), ())),
                preferred_element_type=jnp.float32,
            ).astype(jnp.bfloat16)

    def first(t, carry):
        lesser(batch * t + 1)
        return carry

    lax.fori_loop(0, lag // batch, first, 0)

    load_coup.wait()
    load_occ.wait()
    load_shift.wait()
    for m in range(modes):
        block = coup_ref[m, 0].astype(jnp.float32)
        adjoint = jnp.concatenate([block, turned(coup_ref[m, 0])], 0).T
        right[m, :lanes] = (adjoint * (occ_ref[m] + 1.0)).astype(jnp.bfloat16)
        right[m, lanes:] = (adjoint * occ_ref[m]).astype(jnp.bfloat16)
    low = lax.broadcasted_iota(jnp.int32, (orb, lanes), 1) < orb
    for m in range(0, modes, 2):
        one = coup_ref[m, 0].astype(jnp.float32)
        two = coup_ref[m + 1, 0].astype(jnp.float32)
        span = slice(m * orb, m * orb + lanes)
        left[:orb, span] = jnp.where(low, one, pltpu.roll(two, orb, 1)).astype(
            jnp.bfloat16
        )
        left[orb:, span] = jnp.where(low, pltpu.roll(one, orb, 1), two).astype(
            jnp.bfloat16
        )

    @pl.when(has_other & (lead == 0))
    def _():
        pl.semaphore_wait(barrier, 2 * size)

        def answer(i, carry):
            pl.semaphore_signal(
                far_sem, inc=1, device_id=(other, i), device_id_type=MESH
            )
            return carry

        lax.fori_loop(0, size, answer, 0)

    @pl.when(jnp.logical_not(has_other & (lead == 0)))
    def _():
        pl.semaphore_wait(barrier, size)

    far_base = 2 * size * (1 - core)
    pair_base = 2 * size * core

    def own_copy(a):
        return pltpu.make_async_remote_copy(
            src_ref=mine.at[a],
            dst_ref=own.at[size + loc],
            send_sem=own_send.at[a],
            recv_sem=ext_recv.at[size + loc],
            device_id=(grp, a),
            device_id_type=MESH,
        )

    def far_copy(a):
        return pltpu.make_async_remote_copy(
            src_ref=mine.at[a],
            dst_ref=ext.at[far_base + loc],
            send_sem=far_send.at[a],
            recv_sem=ext_recv.at[far_base + loc],
            device_id=(other, a),
            device_id_type=MESH,
        )

    def pair_copy(j):
        return pltpu.make_async_remote_copy(
            src_ref=own.at[size + j],
            dst_ref=ext.at[pair_base + j],
            send_sem=pair_send.at[j],
            recv_sem=ext_recv.at[pair_base + j],
            device_id=(partner, loc),
            device_id_type=MESH,
        )

    def arrived(slot):
        pltpu.make_async_remote_copy(
            src_ref=ext.at[slot],
            dst_ref=ext.at[slot],
            send_sem=own_send.at[0],
            recv_sem=ext_recv.at[slot],
            device_id=(partner, loc),
            device_id_type=MESH,
        ).wait_recv()

    def send(t):
        a = turn(t)

        own_copy(a).start()

    def later(t, carry):
        for i in range(batch):
            send(batch * t + 1 - lag + i)
        lesser(batch * t + 1)
        return carry

    def last(t, carry):
        send(t)
        return carry

    lax.fori_loop(lag // batch, size // batch, later, 0)
    lax.fori_loop(size - lag + 1, size, last, 0)
    own[size + loc] = mine[loc]

    def direct(t, carry):
        @pl.when(exports(turn(t)))
        def _():
            far_copy(turn(t)).start()

        return carry

    @pl.when(has_other & (lead == 0))
    def _():
        lax.fori_loop(1, size + 1, direct, 0)

    def source(t):
        return (loc + size - t) % size

    def early(t, carry):
        @pl.when(t > 0)
        def _():
            arrived(size + source(t))

        pair_copy(source(t)).start()
        return carry

    def late(t, carry):
        arrived(size + source(t))
        pair_copy(source(t)).start()
        return carry

    lax.fori_loop(0, size - size // 4, early, 0)

    @pl.when(has_other & (lead == 1))
    def _():
        pl.semaphore_wait(far_sem, size)

        lax.fori_loop(1, size + 1, direct, 0)

    lax.fori_loop(size - size // 4, size, late, 0)

    ext[pl.ds(size, size)] = own[pl.ds(size, size)]

    def give_copy(i):
        return pltpu.make_async_remote_copy(
            src_ref=given.at[i],
            dst_ref=part.at[loc],
            send_sem=give_send.at[i],
            recv_sem=part_recv.at[loc],
            device_id=(other, i),
            device_id_type=MESH,
        )

    def finish(m_blocks, target, first):
        for i in range(chunk):
            parts = jnp.dot(left[...], m_blocks[i], preferred_element_type=jnp.float32)
            value = parts[:orb] + pltpu.roll(parts[orb:], orb, 1) * signs((orb, lanes))
            target[first + i] = value.astype(jnp.bfloat16)

    @pl.when(importer)
    def _():
        def give(q, carry):
            first = ((loc // run + q) % pieces) * chunk
            for m in range(modes):
                start = first + shift_ref[m] + core * (2 * size - 2 * shift_ref[m])
                block = own[pl.ds(start, chunk)].reshape(chunk * orb, lanes)
                product = jnp.dot(
                    block,
                    right[m, pl.ds(core * lanes, lanes)],
                    preferred_element_type=jnp.float32,
                )
                mid[:, m * orb : (m + 1) * orb] = product.astype(
                    jnp.bfloat16
                ).reshape(chunk, orb, lanes)
            finish(mid, given, first)
            for i in range(chunk):
                give_copy(first + i).start()
            return carry

        lax.fori_loop(0, pieces, give, 0)

    def halo(j, carry):
        arrived(pair_other + j)

        @pl.when(importer)
        def _():
            arrived(far_other + j)

        return carry

    pair_other = 2 * size * (1 - core)
    far_other = 2 * size * core
    lax.fori_loop(0, size, halo, 0)

    @pl.when(jnp.logical_not(importer))
    def _():
        ext[pl.ds(far_other, size)] = jnp.zeros((size, orb, lanes), ext.dtype)

    def ret_copy(i):
        return pltpu.make_async_remote_copy(
            src_ref=res.at[i],
            dst_ref=out_ref.at[0, loc],
            send_sem=ret_send.at[i],
            recv_sem=out_recv.at[loc],
            device_id=(grp, i),
            device_id_type=MESH,
        )

    def mix(q, carry):
        first = ((loc // run + q) % pieces) * chunk
        for m in range(modes):
            above = ext[pl.ds(size + first + shift_ref[m], chunk)]
            below = ext[pl.ds(size + first - shift_ref[m], chunk)]
            both = jnp.concatenate(
                [above.reshape(chunk * orb, lanes), below.reshape(chunk * orb, lanes)], 1
            )
            product = jnp.dot(both, right[m], preferred_element_type=jnp.float32)
            mid[:, m * orb : (m + 1) * orb] = product.astype(jnp.bfloat16).reshape(
                chunk, orb, lanes
            )
        finish(mid, res, first)
        for i in range(chunk):

            @pl.when(first + i != loc)
            def _():
                ret_copy(first + i).start()

        return carry

    lax.fori_loop(0, pieces, mix, 0)
    out_ref[0, loc] = res[loc]

    def sent(i, carry):
        @pl.when(i != loc)
        def _():
            own_copy(i).wait_send()
            ret_copy(i).wait_send()

        @pl.when(has_other & exports(i))
        def _():
            far_copy(i).wait_send()

        @pl.when(importer)
        def _():
            give_copy(i).wait_send()

        pair_copy(i).wait_send()
        return carry

    lax.fori_loop(0, size, sent, 0)

    def settle(t, carry):
        i = turn(t)

        @pl.when(t > 0)
        def _():
            pltpu.make_async_remote_copy(
                src_ref=res.at[i],
                dst_ref=out_ref.at[0, i],
                send_sem=ret_send.at[i],
                recv_sem=out_recv.at[i],
                device_id=(partner, loc),
                device_id_type=MESH,
            ).wait_recv()

        @pl.when(has_other & exports(i))
        def _():
            pltpu.make_async_remote_copy(
                src_ref=given.at[i],
                dst_ref=part.at[i],
                send_sem=give_send.at[i],
                recv_sem=part_recv.at[i],
                device_id=(partner, loc),
                device_id_type=MESH,
            ).wait_recv()
            total = out_ref[0, i].astype(jnp.float32) + part[i].astype(jnp.float32)
            out_ref[0, i] = total.astype(jnp.bfloat16)

        return carry

    lax.fori_loop(0, size, settle, 0)


def solution(mesh):
    groups = mesh.shape["egrp"]

    def step(green_blocks, sigma_prev, neighbours, couplings, occupancy, shifts):
        _, atoms, hops, orb, lanes = green_blocks.shape
        modes = couplings.shape[0]
        size = atoms
        vmem = pl.BlockSpec(memory_space=pltpu.VMEM)
        hbm = pl.BlockSpec(memory_space=pl.ANY)
        half = jnp.bfloat16
        return pl.pallas_call(
            functools.partial(kernel, groups),
            out_shape=pltpu.VMEM((1, atoms, orb, lanes), half),
            in_specs=[hbm] * 6,
            out_specs=vmem,
            scratch_shapes=[
                pltpu.SMEM(neighbours.shape[::-1], jnp.int32),
                pltpu.SMEM((modes,), jnp.float32),
                pltpu.SMEM((modes,), jnp.int32),
                pltpu.VMEM((atoms, hops, orb, lanes), half),
                pltpu.VMEM((atoms, orb, lanes), half),
                pltpu.VMEM(couplings.shape, half),
                pltpu.VMEM((atoms, lanes, lanes), half),
                pltpu.VMEM((atoms, orb, lanes), half),
                pltpu.VMEM((3 * size, orb, lanes), half),
                pltpu.VMEM((3 * size, orb, lanes), half),
                pltpu.VMEM((modes, 2 * lanes, lanes), half),
                pltpu.VMEM((lanes, modes * orb), half),
                pltpu.VMEM((min(8, size // 2), modes * orb, lanes), half),
                pltpu.VMEM((size, orb, lanes), half),
                pltpu.VMEM((size, orb, lanes), half),
                pltpu.VMEM((size, orb, lanes), half),
                pltpu.SemaphoreType.DMA((atoms + 5,)),
                pltpu.SemaphoreType.DMA((size,)),
                pltpu.SemaphoreType.DMA((size,)),
                pltpu.SemaphoreType.DMA((size,)),
                pltpu.SemaphoreType.DMA((size,)),
                pltpu.SemaphoreType.DMA((3 * size,)),
                pltpu.SemaphoreType.DMA((size,)),
                pltpu.SemaphoreType.DMA((size,)),
                pltpu.SemaphoreType.DMA((size,)),
                pltpu.SemaphoreType.REGULAR,
            ],
            compiler_params=pltpu.CompilerParams(
                collective_id=0, has_side_effects=True
            ),
        )(neighbours.T, occupancy, shifts, green_blocks, sigma_prev, couplings)

    return jax.shard_map(
        step,
        mesh=mesh,
        in_specs=(
            P(("egrp", "eloc"), None, None, None, None),
            P(("egrp", "eloc"), None, None, None),
            P(),
            P(None, "eloc", None, None),
            P(),
            P(),
        ),
        out_specs=P(("egrp", "eloc"), None, None, None),
        check_vma=False,
    )
```
